256 devices in a mesh: vec: 128 (over y, x, z), ao: 2 (over core).
Axes of the slice: x: 4, y: 4, z: 8, core: 2. Of those that a mesh axis runs over, the one named last changes fastest.
Arguments:
- cholesky: float32 [128, 1200, 1200], P('vec', 'ao'), may hold values from -6 to 6
- coefficients: float32 [2, 720000], P('ao', 'vec'), may hold values from -0.1875 to 0.1875
Outputs:
- mo_vectors: float32 [128, 128, 1072], P(None, 'vec', 'ao')
The draws below stay inside these ranges and needn't reach their ends.
All inputs are finite; a program needn't handle non-finite values.
Results may differ from the reference program's by a relative error of at most 0.0001.
Values sent between devices are 32-bit elements; how exact they have to be, the bound alone decides.
No kernel may reach another device: no remote copies, remote signals or barrier semaphores. Data moves between devices by JAX's collectives and lax.ppermute only.
A program may use at most 64 MiB of HBM per device.

```python
import jax
import jax.numpy as jnp
from jax import lax

NAO = 1200
NOCC = 128
NVIR = 1072
NMO = 1200
HALF_AO = 600
NVEC = 128
N_AO = 2


def steps_of(key, shape, split, low, top_value):
    level, own = 1.0, jax.random.fold_in(key, 6)
    for position, blocks in split:
        steps = jnp.exp(jax.random.uniform(jax.random.fold_in(own, position), (blocks,), jnp.float32, low / len(split), top_value / len(split)))
        level = level * jnp.repeat(steps, shape[position] // blocks).reshape([-1 if axis == position else 1 for axis in range(len(shape))])
    return level


def bell_draw(stream_key, extent, width, most, split=(), kind=jnp.bfloat16):
    entries = width * jax.random.normal(stream_key, extent, jnp.float32)
    if split:
        entries = entries * steps_of(stream_key, extent, split, -0.22, 0.18)
    return jnp.clip(entries, -most, most).astype(kind)


def setup_inputs(seed: int = 0) -> dict:
    streams_of = jax.random.split(jax.random.key(seed), 3)
    cholesky = bell_draw(streams_of[0], (NVEC, NAO, NAO), 1.0, 6.0, ((0, 128), (1, 2)), jnp.float32)
    coefficients = bell_draw(streams_of[1], (N_AO, HALF_AO * NMO), NAO ** -0.5, 0.1875, ((0, 2), (1, 128)), jnp.float32)
    return dict(cholesky=cholesky, coefficients=coefficients)


def reference(cholesky, coefficients):
    matrix = coefficients.reshape(NAO, NOCC + NVIR)
    occupied = matrix[:, :NOCC]
    virtual = matrix[:, NOCC:]

    def transform_one(vector):
        left_half = jnp.dot(occupied.T, vector, precision=lax.Precision.HIGHEST, preferred_element_type=jnp.float32)
        return jnp.dot(left_half, virtual, precision=lax.Precision.HIGHEST, preferred_element_type=jnp.float32)

    return lax.map(transform_one, cholesky)
```

```python
import functools

import jax
import jax.numpy as jnp
from jax import lax
from jax.experimental import pallas as pl
from jax.experimental.pallas import tpu as pltpu
from jax.sharding import Mesh
from jax.sharding import PartitionSpec as P

VEC = ("vec_0", "vec_1", "vec_2")
LANES = 128
F32, BF16 = jnp.float32, jnp.bfloat16

NAO, NOCC, NVIR = 1200, 128, 1072
HALF = 600
HALF_PAD = 640
HALF_VIR = 536
SHARD = 5625
SHARD_ROWS = 44
SHARD_PAD = SHARD_ROWS * LANES
GROUP = 16
GROUP_ROWS = 75
BLOCKS = 11
VMEM = pl.BlockSpec(memory_space=pltpu.VMEM)


def hi_lo(x):
    hi = x.astype(BF16)
    return hi, (x - hi.astype(F32)).astype(BF16)


def prepare_kernel(chol, hi_out, lo_out):
    for h in range(2):
        part = chol[0, :, h * HALF : (h + 1) * HALF]
        part = jnp.concatenate([part, jnp.zeros((HALF, HALF_PAD - HALF), F32)], axis=1)
        part = jnp.concatenate([part, jnp.zeros((HALF_PAD - HALF, HALF_PAD), F32)], axis=0)
        hi, lo = hi_lo(part)
        hi_out[h], lo_out[h] = hi, lo


def prepare(chol):
    shape = jax.ShapeDtypeStruct((2, HALF_PAD, HALF_PAD), BF16)
    return pl.pallas_call(
        prepare_kernel,
        out_shape=(shape, shape),
        in_specs=[VMEM],
        out_specs=(VMEM, VMEM),
        cost_estimate=pl.CostEstimate(flops=20_000_000, bytes_accessed=6_000_000, transcendentals=0),
        name="prepare",
    )(chol)


def rows_kernel(raw, chol_hi, chol_lo, table, keep, send):
    lane = lax.broadcasted_iota(jnp.int32, (8, LANES), 1)
    place = lax.broadcasted_iota(jnp.int32, (8, LANES), 0) * LANES + lane

    def piece(base, shard, start):
        at = shard * SHARD_ROWS + start // LANES
        shift = start % LANES
        last = GROUP * SHARD_ROWS - 8
        if at > last:
            block = pltpu.roll(raw[pl.ds(base + last, 8), :], 8 - (at - last), 0)
        else:
            block = raw[pl.ds(base + at, 8), :]
        if shift == 0:
            return block
        turned = pltpu.roll(block, LANES - shift, 1)
        return jnp.where(lane < LANES - shift, turned, pltpu.roll(turned, 7, 0))

    def group(g, carry):
        base = pl.multiple_of(g * (GROUP * SHARD_ROWS), 8)
        for r in range(GROUP_ROWS):
            for first, column, blocks in ((0, 0, 6), (6, NOCC + HALF_VIR, 5)):
                flat = r * NAO + column
                end = flat + min(blocks * LANES, NAO - column)
                shard = flat // SHARD
                start = flat - shard * SHARD
                value = piece(base, shard, start)
                if end > (shard + 1) * SHARD:
                    other = piece(base, shard + 1, start - SHARD)
                    value = jnp.where(place < SHARD - start, value, other)
                table[pl.ds(first * HALF_PAD + g * GROUP_ROWS + r, blocks, stride=HALF_PAD), :] = value[:blocks]
        return carry

    lax.fori_loop(0, 8, group, 0)
    for j in range(BLOCKS):
        table[pl.ds(j * HALF_PAD + HALF, HALF_PAD - HALF), :] = jnp.zeros((HALF_PAD - HALF, LANES), F32)

    hi, lo = hi_lo(table[0:HALF_PAD, :].T)
    both = jnp.concatenate([hi, lo], axis=0)
    own = lax.axis_index("ao")
    for h in range(2):
        part = jnp.dot(both, chol_hi[h], preferred_element_type=F32)
        part = part[:NOCC] + part[NOCC:] + jnp.dot(hi, chol_lo[h], preferred_element_type=F32)

        @pl.when(own == h)
        def _():
            keep[...] = part

        @pl.when(own != h)
        def _():
            send[...] = part


def rows_and_first(raw, chol_hi, chol_lo):
    half = jax.ShapeDtypeStruct((NOCC, HALF_PAD), F32)
    return pl.pallas_call(
        rows_kernel,
        out_shape=(jax.ShapeDtypeStruct((BLOCKS * HALF_PAD, LANES), F32), half, half),
        in_specs=[VMEM] * 3,
        out_specs=(VMEM,) * 3,
        cost_estimate=pl.CostEstimate(flops=600_000_000, bytes_accessed=10_000_000, transcendentals=0),
        name="rows_and_first",
    )(raw, chol_hi, chol_lo)


def split_kernel(table, hi_out, lo_out):
    for j in range(1, BLOCKS):
        hi, lo = hi_lo(table[j * HALF_PAD : (j + 1) * HALF_PAD, :])
        columns = pl.ds((j - 1) * LANES, LANES)
        hi_out[:, columns] = hi
        lo_out[:, columns] = lo


def split(table):
    shape = jax.ShapeDtypeStruct((HALF_PAD, 2 * HALF_PAD), BF16)
    return pl.pallas_call(
        split_kernel,
        out_shape=(shape, shape),
        in_specs=[VMEM],
        out_specs=(VMEM, VMEM),
        cost_estimate=pl.CostEstimate(flops=20_000_000, bytes_accessed=6_000_000, transcendentals=0),
        name="split",
    )(table)


def second_kernel(kept, came, vir_hi, vir_lo, keep, send):
    hi, lo = hi_lo(kept[...] + came[...])
    both = jnp.concatenate([hi, lo], axis=0)
    own = lax.axis_index("ao")
    for h in range(2):
        columns = pl.ds(h * HALF_PAD, HALF_PAD)
        part = jnp.dot(both, vir_hi[:, columns], preferred_element_type=F32)
        part = part[:NOCC] + part[NOCC:] + jnp.dot(hi, vir_lo[:, columns], preferred_element_type=F32)

        @pl.when(own == h)
        def _():
            keep[...] = part

        @pl.when(own != h)
        def _():
            send[...] = part


def second(kept, came, vir_hi, vir_lo):
    half = jax.ShapeDtypeStruct((NOCC, HALF_PAD), F32)
    return pl.pallas_call(
        second_kernel,
        out_shape=(half, half),
        in_specs=[VMEM] * 4,
        out_specs=(VMEM,) * 2,
        cost_estimate=pl.CostEstimate(flops=600_000_000, bytes_accessed=6_000_000, transcendentals=0),
        name="second",
    )(kept, came, vir_hi, vir_lo)


def to_everyone(x, axes, peers):
    return lax.all_to_all(jnp.broadcast_to(x[None], (peers, *x.shape)), axes, 0, 0, tiled=True)


def swap(x):
    return lax.ppermute(x, "ao", [(0, 1), (1, 0)])


def body(cholesky, coefficients):
    shard = jnp.pad(coefficients[0], (0, SHARD_PAD - SHARD))
    line = to_everyone(shard, "vec_2", 8)
    raw = to_everyone(line.reshape(8 * SHARD_ROWS, LANES), ("vec_0", "vec_1"), 16)
    raw = raw.reshape(128 * SHARD_ROWS, LANES)
    chol_hi, chol_lo = prepare(cholesky)
    table, keep, send = rows_and_first(raw, chol_hi, chol_lo)
    came = swap(send)
    vir_hi, vir_lo = split(table)
    keep, send = second(keep, came, vir_hi, vir_lo)
    mine = keep + swap(send)
    owned = lax.all_to_all(mine, VEC, 0, 0, tiled=True)
    return owned[:, None, :HALF_VIR]


def solution(mesh):
    split_mesh = Mesh(mesh.devices.reshape(4, 4, 8, mesh.shape["ao"]), (*VEC, "ao"))
    in_specs = (P(VEC, "ao", None), P("ao", VEC))
    out_specs = P(None, VEC, "ao")
    return jax.shard_map(body, mesh=split_mesh, in_specs=in_specs, out_specs=out_specs, check_vma=False)
```

```python
import functools

import jax
import jax.numpy as jnp
from jax import lax
from jax.experimental import pallas as pl
from jax.experimental.pallas import tpu as pltpu
from jax.sharding import Mesh
from jax.sharding import PartitionSpec as P

VEC = ("vec_0", "vec_1", "vec_2")
LANES = 128
F32, BF16 = jnp.float32, jnp.bfloat16

NAO, NOCC, NVIR = 1200, 128, 1072
HALF = 600
HALF_PAD = 640
HALF_VIR = 536
SHARD = 5625
SHARD_ROWS = 44
SHARD_PAD = SHARD_ROWS * LANES
GROUP = 16
GROUP_ROWS = 75
BLOCKS = 11
VMEM = pl.BlockSpec(memory_space=pltpu.VMEM)


def hi_lo(x):
    hi = x.astype(BF16)
    return hi, (x - hi.astype(F32)).astype(BF16)


def padded_half(chol, h):
    part = chol[0, :, h * HALF : (h + 1) * HALF]
    part = jnp.concatenate([part, jnp.zeros((HALF, HALF_PAD - HALF), F32)], axis=1)
    return jnp.concatenate([part, jnp.zeros((HALF_PAD - HALF, HALF_PAD), F32)], axis=0)


def rows_kernel(raw, chol, table, keep, send):
    lane = lax.broadcasted_iota(jnp.int32, (8, LANES), 1)
    place = lax.broadcasted_iota(jnp.int32, (8, LANES), 0) * LANES + lane

    def piece(base, shard, start):
        at = shard * SHARD_ROWS + start // LANES
        shift = start % LANES
        last = GROUP * SHARD_ROWS - 8
        if at > last:
            block = pltpu.roll(raw[pl.ds(base + last, 8), :], 8 - (at - last), 0)
        else:
            block = raw[pl.ds(base + at, 8), :]
        if shift == 0:
            return block
        turned = pltpu.roll(block, LANES - shift, 1)
        return jnp.where(lane < LANES - shift, turned, pltpu.roll(turned, 7, 0))

    def group(g, carry):
        base = pl.multiple_of(g * (GROUP * SHARD_ROWS), 8)
        for r in range(GROUP_ROWS):
            for first, column, blocks in ((0, 0, 6), (6, NOCC + HALF_VIR, 5)):
                flat = r * NAO + column
                end = flat + min(blocks * LANES, NAO - column)
                shard = flat // SHARD
                start = flat - shard * SHARD
                value = piece(base, shard, start)
                if end > (shard + 1) * SHARD:
                    other = piece(base, shard + 1, start - SHARD)
                    value = jnp.where(place < SHARD - start, value, other)
                table[pl.ds(first * HALF_PAD + g * GROUP_ROWS + r, blocks, stride=HALF_PAD), :] = value[:blocks]
        return carry

    lax.fori_loop(0, 8, group, 0)
    for j in range(BLOCKS):
        table[pl.ds(j * HALF_PAD + HALF, HALF_PAD - HALF), :] = jnp.zeros((HALF_PAD - HALF, LANES), F32)

    hi, lo = hi_lo(table[0:HALF_PAD, :].T)
    both = jnp.concatenate([hi, lo], axis=0)
    own = lax.axis_index("ao")
    for h in range(2):
        chol_hi, chol_lo = hi_lo(padded_half(chol, h))
        part = jnp.dot(both, chol_hi, preferred_element_type=F32)
        part = part[:NOCC] + part[NOCC:] + jnp.dot(hi, chol_lo, preferred_element_type=F32)

        @pl.when(own == h)
        def _():
            keep[...] = part

        @pl.when(own != h)
        def _():
            send[...] = part


def rows_and_first(raw, chol):
    half = jax.ShapeDtypeStruct((NOCC, HALF_PAD), F32)
    return pl.pallas_call(
        rows_kernel,
        out_shape=(jax.ShapeDtypeStruct((BLOCKS * HALF_PAD, LANES), F32), half, half),
        in_specs=[VMEM] * 2,
        out_specs=(VMEM,) * 3,
        cost_estimate=pl.CostEstimate(flops=600_000_000, bytes_accessed=10_000_000, transcendentals=0),
        compiler_params=pltpu.CompilerParams(vmem_limit_bytes=20 * 2**20),
        name="rows_and_first",
    )(raw, chol)


def split_kernel(table, hi_out, lo_out):
    for j in range(1, BLOCKS):
        hi, lo = hi_lo(table[j * HALF_PAD : (j + 1) * HALF_PAD, :])
        columns = pl.ds((j - 1) * LANES, LANES)
        hi_out[:, columns] = hi
        lo_out[:, columns] = lo


def split(table):
    shape = jax.ShapeDtypeStruct((HALF_PAD, 2 * HALF_PAD), BF16)
    return pl.pallas_call(
        split_kernel,
        out_shape=(shape, shape),
        in_specs=[VMEM],
        out_specs=(VMEM, VMEM),
        cost_estimate=pl.CostEstimate(flops=20_000_000, bytes_accessed=6_000_000, transcendentals=0),
        compiler_params=pltpu.CompilerParams(vmem_limit_bytes=12 * 2**20),
        name="split",
    )(table)


def second_kernel(kept, came, vir_hi, vir_lo, keep, send):
    hi, lo = hi_lo(kept[...] + came[...])
    both = jnp.concatenate([hi, lo], axis=0)
    own = lax.axis_index("ao")
    for h in range(2):
        columns = pl.ds(h * HALF_PAD, HALF_PAD)
        part = jnp.dot(both, vir_hi[:, columns], preferred_element_type=F32)
        part = part[:NOCC] + part[NOCC:] + jnp.dot(hi, vir_lo[:, columns], preferred_element_type=F32)

        @pl.when(own == h)
        def _():
            keep[...] = part

        @pl.when(own != h)
        def _():
            send[...] = part


def second(kept, came, vir_hi, vir_lo):
    half = jax.ShapeDtypeStruct((NOCC, HALF_PAD), F32)
    return pl.pallas_call(
        second_kernel,
        out_shape=(half, half),
        in_specs=[VMEM] * 4,
        out_specs=(VMEM,) * 2,
        cost_estimate=pl.CostEstimate(flops=600_000_000, bytes_accessed=6_000_000, transcendentals=0),
        compiler_params=pltpu.CompilerParams(vmem_limit_bytes=12 * 2**20),
        name="second",
    )(kept, came, vir_hi, vir_lo)


def to_everyone(x, axes, peers):
    return lax.all_to_all(jnp.broadcast_to(x[None], (peers, *x.shape)), axes, 0, 0, tiled=True)


def swap(x):
    return lax.ppermute(x, "ao", [(0, 1), (1, 0)])


def body(cholesky, coefficients):
    shard = jnp.pad(coefficients[0], (0, SHARD_PAD - SHARD))
    line = to_everyone(shard, "vec_2", 8)
    raw = to_everyone(line.reshape(8 * SHARD_ROWS, LANES), ("vec_0", "vec_1"), 16)
    raw = raw.reshape(128 * SHARD_ROWS, LANES)
    table, keep, send = rows_and_first(raw, cholesky)
    came = swap(send)
    vir_hi, vir_lo = split(table)
    keep, send = second(keep, came, vir_hi, vir_lo)
    mine = keep + swap(send)
    owned = lax.all_to_all(mine, VEC, 0, 0, tiled=True)
    return owned[:, None, :HALF_VIR]


def solution(mesh):
    split_mesh = Mesh(mesh.devices.reshape(4, 4, 8, mesh.shape["ao"]), (*VEC, "ao"))
    in_specs = (P(VEC, "ao", None), P("ao", VEC))
    out_specs = P(None, VEC, "ao")
    return jax.shard_map(body, mesh=split_mesh, in_specs=in_specs, out_specs=out_specs, check_vma=False)
```

```python
import functools

import jax
import jax.numpy as jnp
from jax import lax
from jax.experimental import pallas as pl
from jax.experimental.pallas import tpu as pltpu
from jax.sharding import Mesh
from jax.sharding import PartitionSpec as P

VEC = ("vec_0", "vec_1", "vec_2")
LANES = 128
F32, BF16 = jnp.float32, jnp.bfloat16

NAO, NOCC, NVIR = 1200, 128, 1072
HALF = 600
HALF_PAD = 640
HALF_VIR = 536
SHARD = 5625
SHARD_ROWS = 44
SHARD_PAD = SHARD_ROWS * LANES
GROUP = 16
GROUP_ROWS = 75
PITCH = HALF_PAD + 1
LINE = 8
LINE_ROWS = LINE * SHARD_ROWS
BLOCKS = 11
VMEM = pl.BlockSpec(memory_space=pltpu.VMEM)


def plane_groups(swapped):
    lines = []
    for core in range(2):
        along_0 = (core == 0) != swapped
        for fixed in range(4):
            cells = [(k, fixed) if along_0 else (fixed, k) for k in range(4)]
            lines.append([(a * 4 + b) * 2 + core for a, b in cells])
    return lines


def hi_lo(x):
    hi = x.astype(BF16)
    return hi, (x - hi.astype(F32)).astype(BF16)


def padded_half(chol, h):
    part = chol[0, :, h * HALF : (h + 1) * HALF]
    part = jnp.concatenate([part, jnp.zeros((HALF, HALF_PAD - HALF), F32)], axis=1)
    return jnp.concatenate([part, jnp.zeros((HALF_PAD - HALF, HALF_PAD), F32)], axis=0)


def rows_kernel(raw, chol, table, keep, send):
    own = lax.axis_index("ao")
    lane = lax.broadcasted_iota(jnp.int32, (8, LANES), 1)
    place = lax.broadcasted_iota(jnp.int32, (8, LANES), 0) * LANES + lane

    def piece(bases, shard, start):
        base = bases[shard // LINE]
        at = shard % LINE * SHARD_ROWS + start // LANES
        shift = start % LANES
        last = LINE_ROWS - 8
        if at > last:
            block = pltpu.roll(raw[pl.ds(base + last, 8), :], 8 - (at - last), 0)
        else:
            block = raw[pl.ds(base + at, 8), :]
        if shift == 0:
            return block
        turned = pltpu.roll(block, LANES - shift, 1)
        return jnp.where(lane < LANES - shift, turned, pltpu.roll(turned, 7, 0))

    def group(g, carry):
        y, x = g // 2, g % 2 * 2
        place_of = [jnp.where(own == 0, (x + k) * 4 + y, y * 4 + x + k) for k in range(2)]
        bases = [pl.multiple_of(at * LINE_ROWS, 8) for at in place_of]
        for r in range(GROUP_ROWS):
            for first, column, blocks in ((0, 0, 6), (6, NOCC + HALF_VIR, 5)):
                flat = r * NAO + column
                end = flat + min(blocks * LANES, NAO - column)
                shard = flat // SHARD
                start = flat - shard * SHARD
                value = piece(bases, shard, start)
                if end > (shard + 1) * SHARD:
                    other = piece(bases, shard + 1, start - SHARD)
                    value = jnp.where(place < SHARD - start, value, other)
                table[pl.ds(first * PITCH + g * GROUP_ROWS + r, blocks, stride=PITCH), :] = value[:blocks]
        return carry

    lax.fori_loop(0, 8, group, 0)
    for j in range(BLOCKS):
        table[pl.ds(j * PITCH + HALF, HALF_PAD - HALF), :] = jnp.zeros((HALF_PAD - HALF, LANES), F32)

    hi, lo = hi_lo(table[0:HALF_PAD, :].T)
    both = jnp.concatenate([hi, lo], axis=0)
    for h in range(2):
        chol_hi, chol_lo = hi_lo(padded_half(chol, h))
        part = jnp.dot(both, chol_hi, preferred_element_type=F32)
        part = part[:NOCC] + part[NOCC:] + jnp.dot(hi, chol_lo, preferred_element_type=F32)

        @pl.when(own == h)
        def _():
            keep[...] = part

        @pl.when(own != h)
        def _():
            send[...] = part


def rows_and_first(raw, chol):
    half = jax.ShapeDtypeStruct((NOCC, HALF_PAD), F32)
    return pl.pallas_call(
        rows_kernel,
        out_shape=(jax.ShapeDtypeStruct((BLOCKS * PITCH, LANES), F32), half, half),
        in_specs=[VMEM] * 2,
        out_specs=(VMEM,) * 3,
        cost_estimate=pl.CostEstimate(flops=600_000_000, bytes_accessed=10_000_000, transcendentals=0),
        compiler_params=pltpu.CompilerParams(vmem_limit_bytes=20 * 2**20),
        name="rows_and_first",
    )(raw, chol)


def split_kernel(table, hi_out, lo_out):
    for j in range(1, BLOCKS):
        hi, lo = hi_lo(table[j * PITCH : j * PITCH + HALF_PAD, :])
        columns = pl.ds((j - 1) * LANES, LANES)
        hi_out[:, columns] = hi
        lo_out[:, columns] = lo


def split(table):
    shape = jax.ShapeDtypeStruct((HALF_PAD, 2 * HALF_PAD), BF16)
    return pl.pallas_call(
        split_kernel,
        out_shape=(shape, shape),
        in_specs=[VMEM],
        out_specs=(VMEM, VMEM),
        cost_estimate=pl.CostEstimate(flops=20_000_000, bytes_accessed=6_000_000, transcendentals=0),
        compiler_params=pltpu.CompilerParams(vmem_limit_bytes=12 * 2**20),
        name="split",
    )(table)


def second_kernel(kept, came, vir_hi, vir_lo, keep, send):
    hi, lo = hi_lo(kept[...] + came[...])
    both = jnp.concatenate([hi, lo], axis=0)
    own = lax.axis_index("ao")
    for h in range(2):
        columns = pl.ds(h * HALF_PAD, HALF_PAD)
        part = jnp.dot(both, vir_hi[:, columns], preferred_element_type=F32)
        part = part[:NOCC] + part[NOCC:] + jnp.dot(hi, vir_lo[:, columns], preferred_element_type=F32)

        @pl.when(own == h)
        def _():
            keep[...] = part

        @pl.when(own != h)
        def _():
            send[...] = part


def second(kept, came, vir_hi, vir_lo):
    half = jax.ShapeDtypeStruct((NOCC, HALF_PAD), F32)
    return pl.pallas_call(
        second_kernel,
        out_shape=(half, half),
        in_specs=[VMEM] * 4,
        out_specs=(VMEM,) * 2,
        cost_estimate=pl.CostEstimate(flops=600_000_000, bytes_accessed=6_000_000, transcendentals=0),
        compiler_params=pltpu.CompilerParams(vmem_limit_bytes=12 * 2**20),
        name="second",
    )(kept, came, vir_hi, vir_lo)


def to_everyone(x, axes, peers, groups=None):
    copies = jnp.broadcast_to(x[None], (peers, *x.shape)).reshape(-1, x.shape[-1])
    return lax.all_to_all(copies, axes, 0, 0, tiled=True, axis_index_groups=groups)


def swap(x):
    return lax.ppermute(x, "ao", [(0, 1), (1, 0)])


def body(cholesky, coefficients):
    shard = jnp.pad(coefficients, ((0, 0), (0, SHARD_PAD - SHARD)))
    line = to_everyone(shard, "vec_2", LINE)
    plane = ("vec_0", "vec_1", "ao")
    raw = to_everyone(line.reshape(LINE_ROWS, LANES), plane, 4, plane_groups(False))
    raw = to_everyone(raw.reshape(4 * LINE_ROWS, LANES), plane, 4, plane_groups(True))
    raw = raw.reshape(128 * SHARD_ROWS, LANES)
    table, keep, send = rows_and_first(raw, cholesky)
    came = swap(send)
    vir_hi, vir_lo = split(table)
    keep, send = second(keep, came, vir_hi, vir_lo)
    mine = keep + swap(send)
    owned = lax.all_to_all(mine, VEC, 0, 0, tiled=True)
    return owned[:, None, :HALF_VIR]


def solution(mesh):
    split_mesh = Mesh(mesh.devices.reshape(4, 4, 8, mesh.shape["ao"]), (*VEC, "ao"))
    in_specs = (P(VEC, "ao", None), P("ao", VEC))
    out_specs = P(None, VEC, "ao")
    return jax.shard_map(body, mesh=split_mesh, in_specs=in_specs, out_specs=out_specs, check_vma=False)
```

```python
import functools

import jax
import jax.numpy as jnp
from jax import lax
from jax.experimental import pallas as pl
from jax.experimental.pallas import tpu as pltpu
from jax.sharding import Mesh
from jax.sharding import PartitionSpec as P

VEC = ("vec_0", "vec_1", "vec_2")
LANES = 128
F32, BF16 = jnp.float32, jnp.bfloat16

NAO, NOCC, NVIR = 1200, 128, 1072
HALF = 600
HALF_PAD = 640
HALF_VIR = 536
SHARD = 5625
SHARD_ROWS = 44
SHARD_PAD = SHARD_ROWS * LANES
GROUP = 16
GROUP_ROWS = 75
PITCH = HALF_PAD + 1
LINE = 8
LINE_ROWS = LINE * SHARD_ROWS
HALF_BLOCKS = 5
VMEM = pl.BlockSpec(memory_space=pltpu.VMEM)


def plane_groups(swapped):
    lines = []
    for core in range(2):
        along_0 = (core == 0) != swapped
        for fixed in range(4):
            cells = [(k, fixed) if along_0 else (fixed, k) for k in range(4)]
            lines.append([(a * 4 + b) * 2 + core for a, b in cells])
    return lines


def hi_lo(x):
    hi = x.astype(BF16)
    return hi, (x - hi.astype(F32)).astype(BF16)


def padded_half(chol, h):
    part = chol[0, :, h * HALF : (h + 1) * HALF]
    part = jnp.concatenate([part, jnp.zeros((HALF, HALF_PAD - HALF), F32)], axis=1)
    return jnp.concatenate([part, jnp.zeros((HALF_PAD - HALF, HALF_PAD), F32)], axis=0)


def each_row(raw, column, columns, store):
    own = lax.axis_index("ao")
    lane = lax.broadcasted_iota(jnp.int32, (8, LANES), 1)
    place = lax.broadcasted_iota(jnp.int32, (8, LANES), 0) * LANES + lane

    def piece(bases, shard, start):
        base = bases[shard // LINE]
        at = shard % LINE * SHARD_ROWS + start // LANES
        shift = start % LANES
        last = LINE_ROWS - 8
        if at > last:
            block = pltpu.roll(raw[pl.ds(base + last, 8), :], 8 - (at - last), 0)
        else:
            block = raw[pl.ds(base + at, 8), :]
        if shift == 0:
            return block
        turned = pltpu.roll(block, LANES - shift, 1)
        return jnp.where(lane < LANES - shift, turned, pltpu.roll(turned, 7, 0))

    def group(g, carry):
        y, x = g // 2, g % 2 * 2
        place_of = [jnp.where(own == 0, (x + k) * 4 + y, y * 4 + x + k) for k in range(2)]
        bases = [pl.multiple_of(at * LINE_ROWS, 8) for at in place_of]
        for r in range(GROUP_ROWS):
            flat = r * NAO + column
            shard = flat // SHARD
            start = flat - shard * SHARD
            value = piece(bases, shard, start)
            if start + columns > SHARD:
                other = piece(bases, shard + 1, start - SHARD)
                value = jnp.where(place < SHARD - start, value, other)
            store(g * GROUP_ROWS + r, value)
        return carry

    lax.fori_loop(0, 8, group, 0)


def three_products(both, hi, lo):
    part = jnp.dot(both, hi, preferred_element_type=F32)
    return part[:NOCC] + part[NOCC:] + jnp.dot(both[:NOCC], lo, preferred_element_type=F32)


def for_half(mine, out, compute):
    own = lax.axis_index("ao")
    for h in range(2):

        @pl.when((own == h) if mine else (own != h))
        def _():
            out[...] = compute(h)


def first_half(both, chol, h):
    return three_products(both, *hi_lo(padded_half(chol, h)))


def occupied_rows(raw, occupied, core):
    lane = lax.broadcasted_iota(jnp.int32, (8, LANES), 1)

    def lines(line, at):
        parts = []
        for h in range(2):
            start, stride = ((2 * h + line) * 4, 1) if core == 0 else (2 * h + line, 4)
            parts.append(raw[pl.ds(start * LINE_ROWS + at, 4, stride=stride * LINE_ROWS), :])
        return jnp.concatenate(parts, axis=0)

    def piece(shard, start):
        at = shard % LINE * SHARD_ROWS + start // LANES
        shift = start % LANES
        rows = [lines(shard // LINE, min(max(q, 0), LINE_ROWS - 1)) for q in (at, at + 1)]
        if shift == 0:
            return rows[0]
        low, high = (pltpu.roll(q, LANES - shift, 1) for q in rows)
        return jnp.where(lane < LANES - shift, low, high)

    for r in range(GROUP_ROWS):
        shard = r * NAO // SHARD
        start = r * NAO - shard * SHARD
        value = piece(shard, start)
        if start + NOCC > SHARD:
            value = jnp.where(lane < SHARD - start, value, piece(shard + 1, start - SHARD))
        for h in range(2):
            occupied[pl.ds(h * GROUP_ROWS + r, 4, stride=2 * GROUP_ROWS), :] = value[4 * h : 4 * h + 4]


def occupied_kernel(raw, chol, both_out, send, occupied):
    own = lax.axis_index("ao")
    for core in range(2):

        @pl.when(own == core)
        def _():
            occupied_rows(raw, occupied, core)

    occupied[HALF:, :] = jnp.zeros((HALF_PAD - HALF, LANES), F32)
    both = jnp.concatenate(hi_lo(occupied[...].T), axis=0)
    both_out[...] = both
    for_half(False, send, lambda h: first_half(both, chol, h))


def virtual_rows(raw, table, mine):
    own = lax.axis_index("ao")

    def store(row, value):
        table[pl.ds(row, HALF_BLOCKS, stride=PITCH), :] = value[:HALF_BLOCKS]

    for h in range(2):

        @pl.when((own == h) if mine else (own != h))
        def _():
            each_row(raw, NOCC + h * HALF_VIR, HALF_VIR, store)

    for j in range(HALF_BLOCKS):
        table[pl.ds(j * PITCH + HALF, PITCH - HALF), :] = jnp.zeros((PITCH - HALF, LANES), F32)


def second_half(both, table):
    blocks = [table[j * PITCH : j * PITCH + HALF_PAD, :] for j in range(HALF_BLOCKS)]
    return three_products(both, *hi_lo(jnp.concatenate(blocks, axis=1)))


def middle_kernel(raw, chol, both, table, keep):
    virtual_rows(raw, table, False)
    for_half(True, keep, lambda h: first_half(both[...], chol, h))


def leaving_kernel(kept, came, table, both_out, send):
    both = jnp.concatenate(hi_lo(kept[...] + came[...]), axis=0)
    both_out[...] = both
    send[...] = second_half(both, table)


def staying_kernel(raw, both, keep, table):
    virtual_rows(raw, table, True)
    keep[...] = second_half(both[...], table)


def call(kernel, outs, *args, scratch=(), mib=16):
    return pl.pallas_call(
        kernel,
        out_shape=outs,
        in_specs=[VMEM] * len(args),
        out_specs=(VMEM,) * len(outs),
        scratch_shapes=scratch,
        compiler_params=pltpu.CompilerParams(vmem_limit_bytes=mib * 2**20),
        cost_estimate=pl.CostEstimate(flops=600_000_000, bytes_accessed=6_000_000, transcendentals=0),
        name=kernel.__name__,
    )(*args)


def to_everyone(x, axes, peers, groups=None):
    copies = jnp.broadcast_to(x[None], (peers, *x.shape)).reshape(-1, x.shape[-1])
    return lax.all_to_all(copies, axes, 0, 0, tiled=True, axis_index_groups=groups)


def swap(x):
    return lax.ppermute(x, "ao", [(0, 1), (1, 0)])


def body(cholesky, coefficients):
    shard = jnp.pad(coefficients, ((0, 0), (0, SHARD_PAD - SHARD)))
    line = to_everyone(shard, "vec_2", LINE)
    plane = ("vec_0", "vec_1", "ao")
    raw = to_everyone(line.reshape(LINE_ROWS, LANES), plane, 4, plane_groups(False))
    raw = to_everyone(raw.reshape(4 * LINE_ROWS, LANES), plane, 4, plane_groups(True))
    raw = raw.reshape(128 * SHARD_ROWS, LANES)
    half = jax.ShapeDtypeStruct((NOCC, HALF_PAD), F32)
    stacked = jax.ShapeDtypeStruct((2 * NOCC, HALF_PAD), BF16)
    table_like = jax.ShapeDtypeStruct((HALF_BLOCKS * PITCH, LANES), F32)
    occupied = pltpu.VMEM((HALF_PAD, LANES), F32)
    both, send = call(occupied_kernel, (stacked, half), raw, cholesky, scratch=(occupied,))
    came = swap(send)
    table, keep = call(middle_kernel, (table_like, half), raw, cholesky, both)
    both, send = call(leaving_kernel, (stacked, half), keep, came, table)
    came = swap(send)
    own_table = pltpu.VMEM(table_like.shape, F32)
    (keep,) = call(staying_kernel, (half,), raw, both, scratch=(own_table,))
    mine = keep + came
    owned = lax.all_to_all(mine, VEC, 0, 0, tiled=True)
    return owned[:, None, :HALF_VIR]


def solution(mesh):
    split_mesh = Mesh(mesh.devices.reshape(4, 4, 8, mesh.shape["ao"]), (*VEC, "ao"))
    in_specs = (P(VEC, "ao", None), P("ao", VEC))
    out_specs = P(None, VEC, "ao")
    return jax.shard_map(body, mesh=split_mesh, in_specs=in_specs, out_specs=out_specs, check_vma=False)
```

```python
import functools

import jax
import jax.numpy as jnp
from jax import lax
from jax.experimental import pallas as pl
from jax.experimental.pallas import tpu as pltpu
from jax.sharding import Mesh
from jax.sharding import PartitionSpec as P

VEC = ("vec_0", "vec_1", "vec_2")
LANES = 128
F32, BF16 = jnp.float32, jnp.bfloat16

NAO, NOCC, NVIR = 1200, 128, 1072
HALF = 600
HALF_PAD = 640
HALF_VIR = 536
SHARD = 5625
SHARD_ROWS = 44
SHARD_PAD = SHARD_ROWS * LANES
GROUP = 16
GROUP_ROWS = 75
PITCH = HALF_PAD + 1
LINE = 8
LINE_ROWS = LINE * SHARD_ROWS
HALF_BLOCKS = 5
VMEM = pl.BlockSpec(memory_space=pltpu.VMEM)


def plane_groups(swapped):
    lines = []
    for core in range(2):
        along_0 = (core == 0) != swapped
        for fixed in range(4):
            cells = [(k, fixed) if along_0 else (fixed, k) for k in range(4)]
            lines.append([(a * 4 + b) * 2 + core for a, b in cells])
    return lines


def hi_lo(x):
    hi = x.astype(BF16)
    return hi, (x - hi.astype(F32)).astype(BF16)


def each_row(raw, column, columns, store):
    own = lax.axis_index("ao")
    lane = lax.broadcasted_iota(jnp.int32, (8, LANES), 1)
    place = lax.broadcasted_iota(jnp.int32, (8, LANES), 0) * LANES + lane

    def piece(bases, shard, start):
        base = bases[shard // LINE]
        at = shard % LINE * SHARD_ROWS + start // LANES
        shift = start % LANES
        last = LINE_ROWS - 8
        if at > last:
            block = pltpu.roll(raw[pl.ds(base + last, 8), :], 8 - (at - last), 0)
        else:
            block = raw[pl.ds(base + at, 8), :]
        if shift == 0:
            return block
        turned = pltpu.roll(block, LANES - shift, 1)
        return jnp.where(lane < LANES - shift, turned, pltpu.roll(turned, 7, 0))

    def group(g, carry):
        y, x = g // 2, g % 2 * 2
        place_of = [jnp.where(own == 0, (x + k) * 4 + y, y * 4 + x + k) for k in range(2)]
        bases = [pl.multiple_of(at * LINE_ROWS, 8) for at in place_of]
        for r in range(GROUP_ROWS):
            flat = r * NAO + column
            shard = flat // SHARD
            start = flat - shard * SHARD
            value = piece(bases, shard, start)
            if start + columns > SHARD:
                other = piece(bases, shard + 1, start - SHARD)
                value = jnp.where(place < SHARD - start, value, other)
            store(g * GROUP_ROWS + r, value)
        return carry

    lax.fori_loop(0, 8, group, 0, unroll=4)


def three_products(both, hi, lo):
    part = jnp.dot(both, hi, preferred_element_type=F32)
    return part[:NOCC] + part[NOCC:] + jnp.dot(both[:NOCC], lo, preferred_element_type=F32)


def for_half(mine, out, compute):
    own = lax.axis_index("ao")
    for h in range(2):

        @pl.when((own == h) if mine else (own != h))
        def _():
            out[...] = compute(h)


def first_half(both, chol, h):
    first = h * HALF // LANES * LANES
    end = min(h * HALF + HALF_PAD, NAO)
    part = chol[0, :, first:end]
    rest = -(end - first) % LANES
    if rest:
        part = jnp.concatenate([part, jnp.zeros((HALF, rest), F32)], axis=1)
    part = jnp.concatenate([part, jnp.zeros((HALF_PAD - HALF, part.shape[1]), F32)], axis=0)
    skip = h * HALF - first
    return three_products(both, *hi_lo(part))[:, skip : skip + HALF_PAD]


def occupied_rows(raw, occupied, core):
    lane = lax.broadcasted_iota(jnp.int32, (8, LANES), 1)

    def lines(line, at):
        parts = []
        for h in range(2):
            start, stride = ((2 * h + line) * 4, 1) if core == 0 else (2 * h + line, 4)
            parts.append(raw[pl.ds(start * LINE_ROWS + at, 4, stride=stride * LINE_ROWS), :])
        return jnp.concatenate(parts, axis=0)

    def piece(shard, start):
        at = shard % LINE * SHARD_ROWS + start // LANES
        shift = start % LANES
        rows = [lines(shard // LINE, min(max(q, 0), LINE_ROWS - 1)) for q in (at, at + 1)]
        if shift == 0:
            return rows[0]
        low, high = (pltpu.roll(q, LANES - shift, 1) for q in rows)
        return jnp.where(lane < LANES - shift, low, high)

    for r in range(GROUP_ROWS):
        shard = r * NAO // SHARD
        start = r * NAO - shard * SHARD
        value = piece(shard, start)
        if start + NOCC > SHARD:
            value = jnp.where(lane < SHARD - start, value, piece(shard + 1, start - SHARD))
        for h in range(2):
            occupied[pl.ds(h * GROUP_ROWS + r, 4, stride=2 * GROUP_ROWS), :] = value[4 * h : 4 * h + 4]


def occupied_kernel(raw, chol, both_out, send, occupied):
    own = lax.axis_index("ao")
    for core in range(2):

        @pl.when(own == core)
        def _():
            occupied_rows(raw, occupied, core)

    occupied[HALF:, :] = jnp.zeros((HALF_PAD - HALF, LANES), F32)
    both = jnp.concatenate(hi_lo(occupied[...].T), axis=0)
    both_out[...] = both
    for_half(False, send, lambda h: first_half(both, chol, h))


def virtual_rows(raw, table, mine):
    own = lax.axis_index("ao")

    def store(row, value):
        table[pl.ds(row, HALF_BLOCKS, stride=PITCH), :] = value[:HALF_BLOCKS]

    for h in range(2):

        @pl.when((own == h) if mine else (own != h))
        def _():
            each_row(raw, NOCC + h * HALF_VIR, HALF_VIR, store)

    for j in range(HALF_BLOCKS):
        table[pl.ds(j * PITCH + HALF, PITCH - HALF), :] = jnp.zeros((PITCH - HALF, LANES), F32)


def second_half(both, table):
    blocks = [table[j * PITCH : j * PITCH + HALF_PAD, :] for j in range(HALF_BLOCKS)]
    return three_products(both, *hi_lo(jnp.concatenate(blocks, axis=1)))


def store_lines(out, value):
    for j in range(HALF_BLOCKS):
        out[pl.ds(j, NOCC, stride=HALF_BLOCKS), :] = value[:, j * LANES : (j + 1) * LANES]


def middle_kernel(raw, chol, both, table, keep):
    virtual_rows(raw, table, False)
    for_half(True, keep, lambda h: first_half(both[...], chol, h))


def leaving_kernel(kept, came, table, both_out, send):
    both = jnp.concatenate(hi_lo(kept[...] + came[...]), axis=0)
    both_out[...] = both
    store_lines(send, second_half(both, table))


def staying_kernel(raw, both, keep, table):
    virtual_rows(raw, table, True)
    store_lines(keep, second_half(both[...], table))


def call(kernel, outs, *args, scratch=(), mib=16):
    return pl.pallas_call(
        kernel,
        out_shape=outs,
        in_specs=[VMEM] * len(args),
        out_specs=(VMEM,) * len(outs),
        scratch_shapes=scratch,
        compiler_params=pltpu.CompilerParams(vmem_limit_bytes=mib * 2**20),
        cost_estimate=pl.CostEstimate(flops=600_000_000, bytes_accessed=6_000_000, transcendentals=0),
        name=kernel.__name__,
    )(*args)


def to_everyone(x, axes, peers, groups=None):
    copies = jnp.broadcast_to(x[None], (peers, *x.shape)).reshape(-1, x.shape[-1])
    return lax.all_to_all(copies, axes, 0, 0, tiled=True, axis_index_groups=groups)


def swap(x):
    return lax.ppermute(x, "ao", [(0, 1), (1, 0)])


def body(cholesky, coefficients):
    shard = jnp.pad(coefficients, ((0, 0), (0, SHARD_PAD - SHARD)))
    line = to_everyone(shard, "vec_2", LINE)
    plane = ("vec_0", "vec_1", "ao")
    raw = to_everyone(line.reshape(LINE_ROWS, LANES), plane, 4, plane_groups(False))
    raw = to_everyone(raw.reshape(4 * LINE_ROWS, LANES), plane, 4, plane_groups(True))
    raw = raw.reshape(128 * SHARD_ROWS, LANES)
    half = jax.ShapeDtypeStruct((NOCC, HALF_PAD), F32)
    stacked = jax.ShapeDtypeStruct((2 * NOCC, HALF_PAD), BF16)
    table_like = jax.ShapeDtypeStruct((HALF_BLOCKS * PITCH, LANES), F32)
    occupied = pltpu.VMEM((HALF_PAD, LANES), F32)
    both, send = call(occupied_kernel, (stacked, half), raw, cholesky, scratch=(occupied,))
    came = swap(send)
    table, keep = call(middle_kernel, (table_like, half), raw, cholesky, both)
    lines = jax.ShapeDtypeStruct((NOCC * HALF_BLOCKS, LANES), F32)
    both, send = call(leaving_kernel, (stacked, lines), keep, came, table)
    came = swap(send)
    own_table = pltpu.VMEM(table_like.shape, F32)
    (keep,) = call(staying_kernel, (lines,), raw, both, scratch=(own_table,))
    mine = (keep + came).reshape(NOCC, HALF_PAD)
    owned = lax.all_to_all(mine, VEC, 0, 0, tiled=True)
    return owned[:, None, :HALF_VIR]


def solution(mesh):
    split_mesh = Mesh(mesh.devices.reshape(4, 4, 8, mesh.shape["ao"]), (*VEC, "ao"))
    in_specs = (P(VEC, "ao", None), P("ao", VEC))
    out_specs = P(None, VEC, "ao")
    return jax.shard_map(body, mesh=split_mesh, in_specs=in_specs, out_specs=out_specs, check_vma=False)
```

```python
import functools

import jax
import jax.numpy as jnp
from jax import lax
from jax.experimental import pallas as pl
from jax.experimental.pallas import tpu as pltpu
from jax.sharding import Mesh
from jax.sharding import PartitionSpec as P

VEC = ("vec_0", "vec_1", "vec_2")
LANES = 128
F32, BF16 = jnp.float32, jnp.bfloat16

NAO, NOCC, NVIR = 1200, 128, 1072
HALF = 600
HALF_PAD = 640
HALF_VIR = 536
SHARD = 5625
SHARD_ROWS = 44
SHARD_PAD = SHARD_ROWS * LANES
GROUP = 16
GROUP_ROWS = 75
PITCH = HALF_PAD + 1
LINE = 8
LINE_ROWS = LINE * SHARD_ROWS
HALF_BLOCK = 2 * LINE_ROWS
HALF_BLOCKS = 5
VMEM = pl.BlockSpec(memory_space=pltpu.VMEM)


def plane_groups(swapped):
    lines = []
    for core in range(2):
        along_0 = (core == 0) != swapped
        for fixed in range(4):
            cells = [(k, fixed) if along_0 else (fixed, k) for k in range(4)]
            lines.append([(a * 4 + b) * 2 + core for a, b in cells])
    return lines


def shift_pairs(step):
    pairs = []
    for a in range(4):
        for b in range(4):
            pairs.append(((a * 4 + b) * 2, (a * 4 + (b + step) % 4) * 2))
            pairs.append(((a * 4 + b) * 2 + 1, ((a + step) % 4 * 4 + b) * 2 + 1))
    return pairs


def hi_lo(x):
    hi = x.astype(BF16)
    return hi, (x - hi.astype(F32)).astype(BF16)


def each_row(raw, column, columns, store):
    own = lax.axis_index("ao")
    lane = lax.broadcasted_iota(jnp.int32, (8, LANES), 1)
    place = lax.broadcasted_iota(jnp.int32, (8, LANES), 0) * LANES + lane

    def piece(bases, shard, start):
        base = bases[shard // LINE]
        at = shard % LINE * SHARD_ROWS + start // LANES
        shift = start % LANES
        last = LINE_ROWS - 8
        if at > last:
            block = pltpu.roll(raw[pl.ds(base + last, 8), :], 8 - (at - last), 0)
        else:
            block = raw[pl.ds(base + at, 8), :]
        if shift == 0:
            return block
        turned = pltpu.roll(block, LANES - shift, 1)
        return jnp.where(lane < LANES - shift, turned, pltpu.roll(turned, 7, 0))

    def group(g, carry):
        y, x = g // 2, g % 2 * 2
        place_of = [jnp.where(own == 0, (x + k) * 4 + y, y * 4 + x + k) for k in range(2)]
        bases = [pl.multiple_of(at * LINE_ROWS, 8) for at in place_of]
        for r in range(GROUP_ROWS):
            flat = r * NAO + column
            shard = flat // SHARD
            start = flat - shard * SHARD
            value = piece(bases, shard, start)
            if start + columns > SHARD:
                other = piece(bases, shard + 1, start - SHARD)
                value = jnp.where(place < SHARD - start, value, other)
            store(g * GROUP_ROWS + r, value)
        return carry

    lax.fori_loop(0, 8, group, 0, unroll=4)


def three_products(both, hi, lo):
    part = jnp.dot(both, hi, preferred_element_type=F32)
    return part[:NOCC] + part[NOCC:] + jnp.dot(both[:NOCC], lo, preferred_element_type=F32)


def for_half(mine, out, compute):
    own = lax.axis_index("ao")
    for h in range(2):

        @pl.when((own == h) if mine else (own != h))
        def _():
            out[...] = compute(h)


def first_half(both, chol, h):
    first = h * HALF // LANES * LANES
    end = min(h * HALF + HALF_PAD, NAO)
    part = chol[0, :, first:end]
    rest = -(end - first) % LANES
    if rest:
        part = jnp.concatenate([part, jnp.zeros((HALF, rest), F32)], axis=1)
    part = jnp.concatenate([part, jnp.zeros((HALF_PAD - HALF, part.shape[1]), F32)], axis=0)
    skip = h * HALF - first
    return three_products(both, *hi_lo(part))[:, skip : skip + HALF_PAD]


def occupied_rows(raw, occupied, core):
    lane = lax.broadcasted_iota(jnp.int32, (8, LANES), 1)

    def lines(line, at):
        parts = []
        for h in range(2):
            start, stride = ((2 * h + line) * 4, 1) if core == 0 else (2 * h + line, 4)
            parts.append(raw[pl.ds(start * LINE_ROWS + at, 4, stride=stride * LINE_ROWS), :])
        return jnp.concatenate(parts, axis=0)

    def piece(shard, start):
        at = shard % LINE * SHARD_ROWS + start // LANES
        shift = start % LANES
        rows = [lines(shard // LINE, min(max(q, 0), LINE_ROWS - 1)) for q in (at, at + 1)]
        if shift == 0:
            return rows[0]
        low, high = (pltpu.roll(q, LANES - shift, 1) for q in rows)
        return jnp.where(lane < LANES - shift, low, high)

    for r in range(GROUP_ROWS):
        shard = r * NAO // SHARD
        start = r * NAO - shard * SHARD
        value = piece(shard, start)
        if start + NOCC > SHARD:
            value = jnp.where(lane < SHARD - start, value, piece(shard + 1, start - SHARD))
        for h in range(2):
            occupied[pl.ds(h * GROUP_ROWS + r, 4, stride=2 * GROUP_ROWS), :] = value[4 * h : 4 * h + 4]


def occupied_kernel(own_block, left_low, left_high, right_low, right_high, far_low, far_high, chol, raw, both_out, send, occupied):
    own = lax.axis_index("ao")
    here = jnp.where(own == 0, lax.axis_index("vec_1"), lax.axis_index("vec_0"))
    parts = [
        (own_block, 0, 0),
        (left_low, 3, 0),
        (left_high, 3, HALF_BLOCK),
        (right_low, 1, 0),
        (right_high, 1, HALF_BLOCK),
        (far_low, 2, 0),
        (far_high, 2, HALF_BLOCK),
    ]
    for part, step, offset in parts:
        at = (here + step) % 4 * (2 * HALF_BLOCK) + offset
        raw[pl.ds(pl.multiple_of(at, 8), part.shape[0]), :] = part[...]

    for core in range(2):

        @pl.when(own == core)
        def _():
            occupied_rows(raw, occupied, core)

    occupied[HALF:, :] = jnp.zeros((HALF_PAD - HALF, LANES), F32)
    both = jnp.concatenate(hi_lo(occupied[...].T), axis=0)
    both_out[...] = both
    for_half(False, send, lambda h: first_half(both, chol, h))


def virtual_rows(raw, table, mine):
    own = lax.axis_index("ao")

    def store(row, value):
        table[pl.ds(row, HALF_BLOCKS, stride=PITCH), :] = value[:HALF_BLOCKS]

    for h in range(2):

        @pl.when((own == h) if mine else (own != h))
        def _():
            each_row(raw, NOCC + h * HALF_VIR, HALF_VIR, store)

    for j in range(HALF_BLOCKS):
        table[pl.ds(j * PITCH + HALF, PITCH - HALF), :] = jnp.zeros((PITCH - HALF, LANES), F32)


def second_half(both, table):
    blocks = [table[j * PITCH : j * PITCH + HALF_PAD, :] for j in range(HALF_BLOCKS)]
    return three_products(both, *hi_lo(jnp.concatenate(blocks, axis=1)))


def store_lines(out, value):
    for j in range(HALF_BLOCKS):
        out[pl.ds(j, NOCC, stride=HALF_BLOCKS), :] = value[:, j * LANES : (j + 1) * LANES]


def middle_kernel(raw, chol, both, table, keep):
    virtual_rows(raw, table, False)
    for_half(True, keep, lambda h: first_half(both[...], chol, h))


def leaving_kernel(kept, came, table, both_out, send):
    both = jnp.concatenate(hi_lo(kept[...] + came[...]), axis=0)
    both_out[...] = both
    store_lines(send, second_half(both, table))


def staying_kernel(raw, both, keep, table):
    virtual_rows(raw, table, True)
    store_lines(keep, second_half(both[...], table))


def call(kernel, outs, *args, scratch=(), mib=16):
    return pl.pallas_call(
        kernel,
        out_shape=outs,
        in_specs=[VMEM] * len(args),
        out_specs=(VMEM,) * len(outs),
        scratch_shapes=scratch,
        compiler_params=pltpu.CompilerParams(vmem_limit_bytes=mib * 2**20),
        cost_estimate=pl.CostEstimate(flops=600_000_000, bytes_accessed=6_000_000, transcendentals=0),
        name=kernel.__name__,
    )(*args)


def to_everyone(x, axes, peers, groups=None):
    copies = jnp.broadcast_to(x[None], (peers, *x.shape)).reshape(-1, x.shape[-1])
    return lax.all_to_all(copies, axes, 0, 0, tiled=True, axis_index_groups=groups)


def swap(x):
    return lax.ppermute(x, "ao", [(0, 1), (1, 0)])


def body(cholesky, coefficients):
    shard = jnp.pad(coefficients, ((0, 0), (0, SHARD_PAD - SHARD)))
    line = to_everyone(shard, "vec_2", LINE)
    plane = ("vec_0", "vec_1", "ao")
    raw = to_everyone(line.reshape(LINE_ROWS, LANES), plane, 4, plane_groups(False))
    block = raw.reshape(4 * LINE_ROWS, LANES)
    low, high = block[:HALF_BLOCK], block[HALF_BLOCK:]
    left_low = lax.ppermute(low, plane, shift_pairs(1))
    right_high = lax.ppermute(high, plane, shift_pairs(3))
    left_high = lax.ppermute(high, plane, shift_pairs(1))
    right_low = lax.ppermute(low, plane, shift_pairs(3))
    far_low = lax.ppermute(left_low, plane, shift_pairs(1))
    far_high = lax.ppermute(right_high, plane, shift_pairs(3))
    blocks = (block, left_low, left_high, right_low, right_high, far_low, far_high)
    half = jax.ShapeDtypeStruct((NOCC, HALF_PAD), F32)
    stacked = jax.ShapeDtypeStruct((2 * NOCC, HALF_PAD), BF16)
    table_like = jax.ShapeDtypeStruct((HALF_BLOCKS * PITCH, LANES), F32)
    occupied = pltpu.VMEM((HALF_PAD, LANES), F32)
    raw_like = jax.ShapeDtypeStruct((8 * HALF_BLOCK, LANES), F32)
    raw, both, send = call(occupied_kernel, (raw_like, stacked, half), *blocks, cholesky, scratch=(occupied,), mib=20)
    came = swap(send)
    table, keep = call(middle_kernel, (table_like, half), raw, cholesky, both)
    lines = jax.ShapeDtypeStruct((NOCC * HALF_BLOCKS, LANES), F32)
    both, send = call(leaving_kernel, (stacked, lines), keep, came, table)
    came = swap(send)
    own_table = pltpu.VMEM(table_like.shape, F32)
    (keep,) = call(staying_kernel, (lines,), raw, both, scratch=(own_table,))
    mine = (keep + came).reshape(NOCC, HALF_PAD)
    owned = lax.all_to_all(mine, VEC, 0, 0, tiled=True)
    return owned[:, None, :HALF_VIR]


def solution(mesh):
    split_mesh = Mesh(mesh.devices.reshape(4, 4, 8, mesh.shape["ao"]), (*VEC, "ao"))
    in_specs = (P(VEC, "ao", None), P("ao", VEC))
    out_specs = P(None, VEC, "ao")
    return jax.shard_map(body, mesh=split_mesh, in_specs=in_specs, out_specs=out_specs, check_vma=False)
```

```python
import functools

import jax
import jax.numpy as jnp
from jax import lax
from jax.experimental import pallas as pl
from jax.experimental.pallas import tpu as pltpu
from jax.sharding import Mesh
from jax.sharding import PartitionSpec as P

VEC = ("vec_0", "vec_1", "vec_2")
LANES = 128
F32, BF16 = jnp.float32, jnp.bfloat16

NAO, NOCC, NVIR = 1200, 128, 1072
HALF = 600
HALF_PAD = 640
HALF_VIR = 536
SHARD = 5625
SHARD_ROWS = 44
SHARD_PAD = SHARD_ROWS * LANES
GROUP = 16
GROUP_ROWS = 75
PITCH = HALF_PAD + 1
LINE = 8
LINE_ROWS = LINE * SHARD_ROWS
LOW, HIGH = (0, 3), (1, 2)
PLACES = tuple(((last, at[0]), (last, at[1])) for last in (0, 3, 1, 2) for at in (LOW, HIGH))
HALF_BLOCKS = 5
VMEM = pl.BlockSpec(memory_space=pltpu.VMEM)


def pass_on(x, last, step):
    pairs = []
    for a in range(4):
        for b in range(4):
            for core in range(2):
                along_0 = (core == 0) != last
                to = ((a + step) % 4, b) if along_0 else (a, (b + step) % 4)
                pairs.append(((a * 4 + b) * 2 + core, (to[0] * 4 + to[1]) * 2 + core))
    return lax.ppermute(x, ("vec_0", "vec_1", "ao"), pairs)


def hi_lo(x):
    hi = x.astype(BF16)
    return hi, (x - hi.astype(F32)).astype(BF16)


def each_row(raw, column, columns, store):
    own = lax.axis_index("ao")
    lane = lax.broadcasted_iota(jnp.int32, (8, LANES), 1)
    place = lax.broadcasted_iota(jnp.int32, (8, LANES), 0) * LANES + lane

    def piece(bases, shard, start):
        base = bases[shard // LINE]
        at = shard % LINE * SHARD_ROWS + start // LANES
        shift = start % LANES
        last = LINE_ROWS - 8
        if at > last:
            block = pltpu.roll(raw[pl.ds(base + last, 8), :], 8 - (at - last), 0)
        else:
            block = raw[pl.ds(base + at, 8), :]
        if shift == 0:
            return block
        turned = pltpu.roll(block, LANES - shift, 1)
        return jnp.where(lane < LANES - shift, turned, pltpu.roll(turned, 7, 0))

    def group(g, carry):
        y, x = g // 2, g % 2 * 2
        place_of = [jnp.where(own == 0, (x + k) * 4 + y, y * 4 + x + k) for k in range(2)]
        bases = [pl.multiple_of(at * LINE_ROWS, 8) for at in place_of]
        for r in range(GROUP_ROWS):
            flat = r * NAO + column
            shard = flat // SHARD
            start = flat - shard * SHARD
            value = piece(bases, shard, start)
            if start + columns > SHARD:
                other = piece(bases, shard + 1, start - SHARD)
                value = jnp.where(place < SHARD - start, value, other)
            store(g * GROUP_ROWS + r, value)
        return carry

    lax.fori_loop(0, 8, group, 0, unroll=4)


def three_products(both, hi, lo):
    part = jnp.dot(both, hi, preferred_element_type=F32)
    return part[:NOCC] + part[NOCC:] + jnp.dot(both[:NOCC], lo, preferred_element_type=F32)


def for_half(mine, out, compute):
    own = lax.axis_index("ao")
    for h in range(2):

        @pl.when((own == h) if mine else (own != h))
        def _():
            out[...] = compute(h)


def prepare_kernel(chol, *outs):
    for h in range(2):
        first = h * HALF // LANES * LANES
        end = min(h * HALF + HALF_PAD, NAO)
        part = chol[0, :, first:end]
        rest = -(end - first) % LANES
        if rest:
            part = jnp.concatenate([part, jnp.zeros((HALF, rest), F32)], axis=1)
        part = jnp.concatenate([part, jnp.zeros((HALF_PAD - HALF, part.shape[1]), F32)], axis=0)
        outs[2 * h][...], outs[2 * h + 1][...] = hi_lo(part)


def first_half(both, vectors, h):
    skip = h * HALF % LANES
    return three_products(both, vectors[2 * h][...], vectors[2 * h + 1][...])[:, skip : skip + HALF_PAD]


def occupied_rows(raw, occupied, core):
    lane = lax.broadcasted_iota(jnp.int32, (8, LANES), 1)

    def lines(line, at):
        parts = []
        for h in range(2):
            start, stride = ((2 * h + line) * 4, 1) if core == 0 else (2 * h + line, 4)
            parts.append(raw[pl.ds(start * LINE_ROWS + at, 4, stride=stride * LINE_ROWS), :])
        return jnp.concatenate(parts, axis=0)

    def piece(shard, start):
        at = shard % LINE * SHARD_ROWS + start // LANES
        shift = start % LANES
        rows = [lines(shard // LINE, min(max(q, 0), LINE_ROWS - 1)) for q in (at, at + 1)]
        if shift == 0:
            return rows[0]
        low, high = (pltpu.roll(q, LANES - shift, 1) for q in rows)
        return jnp.where(lane < LANES - shift, low, high)

    for r in range(GROUP_ROWS):
        shard = r * NAO // SHARD
        start = r * NAO - shard * SHARD
        value = piece(shard, start)
        if start + NOCC > SHARD:
            value = jnp.where(lane < SHARD - start, value, piece(shard + 1, start - SHARD))
        for h in range(2):
            occupied[pl.ds(h * GROUP_ROWS + r, 4, stride=2 * GROUP_ROWS), :] = value[4 * h : 4 * h + 4]


def occupied_kernel(*refs):
    raw, both_out, send, occupied = refs[-4:]
    blocks, vectors = refs[: len(PLACES)], refs[len(PLACES) : -4]
    own = lax.axis_index("ao")
    along = lax.axis_index("vec_0"), lax.axis_index("vec_1")
    first = jnp.where(own == 0, along[0], along[1])
    last = jnp.where(own == 0, along[1], along[0])
    for block, places in zip(blocks, PLACES):
        for k, (last_step, first_step) in enumerate(places):
            at = (last + last_step) % 4 * 4 + (first + first_step) % 4
            line = block[k * LINE_ROWS : (k + 1) * LINE_ROWS, :]
            raw[pl.ds(pl.multiple_of(at * LINE_ROWS, 8), LINE_ROWS), :] = line

    for core in range(2):

        @pl.when(own == core)
        def _():
            occupied_rows(raw, occupied, core)

    occupied[HALF:, :] = jnp.zeros((HALF_PAD - HALF, LANES), F32)
    both = jnp.concatenate(hi_lo(occupied[...].T), axis=0)
    both_out[...] = both
    for_half(False, send, lambda h: first_half(both, vectors, h))


def virtual_rows(raw, table, mine):
    own = lax.axis_index("ao")

    def store(row, value):
        table[pl.ds(row, HALF_BLOCKS, stride=PITCH), :] = value[:HALF_BLOCKS]

    for h in range(2):

        @pl.when((own == h) if mine else (own != h))
        def _():
            each_row(raw, NOCC + h * HALF_VIR, HALF_VIR, store)

    for j in range(HALF_BLOCKS):
        table[pl.ds(j * PITCH + HALF, PITCH - HALF), :] = jnp.zeros((PITCH - HALF, LANES), F32)


def second_half(both, table):
    blocks = [table[j * PITCH : j * PITCH + HALF_PAD, :] for j in range(HALF_BLOCKS)]
    return three_products(both, *hi_lo(jnp.concatenate(blocks, axis=1)))


def store_lines(out, value):
    for j in range(HALF_BLOCKS):
        out[pl.ds(j, NOCC, stride=HALF_BLOCKS), :] = value[:, j * LANES : (j + 1) * LANES]


def middle_kernel(raw, both, *refs):
    *vectors, table, keep = refs
    virtual_rows(raw, table, False)
    for_half(True, keep, lambda h: first_half(both[...], vectors, h))


def leaving_kernel(kept, came, table, both_out, send):
    both = jnp.concatenate(hi_lo(kept[...] + came[...]), axis=0)
    both_out[...] = both
    store_lines(send, second_half(both, table))


def staying_kernel(raw, both, keep, table):
    virtual_rows(raw, table, True)
    store_lines(keep, second_half(both[...], table))


def call(kernel, outs, *args, scratch=(), mib=16):
    return pl.pallas_call(
        kernel,
        out_shape=outs,
        in_specs=[VMEM] * len(args),
        out_specs=(VMEM,) * len(outs),
        scratch_shapes=scratch,
        compiler_params=pltpu.CompilerParams(vmem_limit_bytes=mib * 2**20),
        cost_estimate=pl.CostEstimate(flops=600_000_000, bytes_accessed=6_000_000, transcendentals=0),
        name=kernel.__name__,
    )(*args)


def to_everyone(x, axes, peers):
    copies = jnp.broadcast_to(x[None], (peers, *x.shape)).reshape(-1, x.shape[-1])
    return lax.all_to_all(copies, axes, 0, 0, tiled=True)


def swap(x):
    return lax.ppermute(x, "ao", [(0, 1), (1, 0)])


def body(cholesky, coefficients):
    shard = jnp.pad(coefficients, ((0, 0), (0, SHARD_PAD - SHARD)))
    line = to_everyone(shard, "vec_2", LINE)
    own = line.reshape(LINE_ROWS, LANES)
    below, above, across = (pass_on(own, False, step) for step in (1, 3, 2))
    own, below, above, across = lax.optimization_barrier((own, below, above, across))
    low = jnp.concatenate([own, below], axis=0)
    high = jnp.concatenate([above, across], axis=0)
    left_low, right_high = pass_on(low, True, 1), pass_on(high, True, 3)
    left_high, right_low = pass_on(high, True, 1), pass_on(low, True, 3)
    far_low, far_high = pass_on(left_low, True, 1), pass_on(right_high, True, 3)
    blocks = (low, high, left_low, left_high, right_low, right_high, far_low, far_high)
    widths = (HALF_PAD, HALF_PAD, HALF_PAD + LANES, HALF_PAD + LANES)
    vectors = call(prepare_kernel, tuple(jax.ShapeDtypeStruct((HALF_PAD, w), BF16) for w in widths), cholesky)
    half = jax.ShapeDtypeStruct((NOCC, HALF_PAD), F32)
    stacked = jax.ShapeDtypeStruct((2 * NOCC, HALF_PAD), BF16)
    table_like = jax.ShapeDtypeStruct((HALF_BLOCKS * PITCH, LANES), F32)
    occupied = pltpu.VMEM((HALF_PAD, LANES), F32)
    raw_like = jax.ShapeDtypeStruct((16 * LINE_ROWS, LANES), F32)
    raw, both, send = call(occupied_kernel, (raw_like, stacked, half), *blocks, *vectors, scratch=(occupied,), mib=20)
    came = swap(send)
    table, keep = call(middle_kernel, (table_like, half), raw, both, *vectors)
    lines = jax.ShapeDtypeStruct((NOCC * HALF_BLOCKS, LANES), F32)
    both, send = call(leaving_kernel, (stacked, lines), keep, came, table)
    came = swap(send)
    own_table = pltpu.VMEM(table_like.shape, F32)
    (keep,) = call(staying_kernel, (lines,), raw, both, scratch=(own_table,))
    mine = (keep + came).reshape(NOCC, HALF_PAD)
    owned = lax.all_to_all(mine, VEC, 0, 0, tiled=True)
    return owned[:, None, :HALF_VIR]


def solution(mesh):
    split_mesh = Mesh(mesh.devices.reshape(4, 4, 8, mesh.shape["ao"]), (*VEC, "ao"))
    in_specs = (P(VEC, "ao", None), P("ao", VEC))
    out_specs = P(None, VEC, "ao")
    return jax.shard_map(body, mesh=split_mesh, in_specs=in_specs, out_specs=out_specs, check_vma=False)
```
